32 devices in a mesh: grp: 4 (over z), dp: 8 (over y, x, core).
Axes of the slice: x: 2, y: 2, z: 4, core: 2. Of those that a mesh axis runs over, the one named last changes fastest.
Arguments:
- tokens: bfloat16 [4096, 3584], P(('grp', 'dp')), may hold values from -120 to 120, as said below
- lengths: int32 [32, 4], P(('grp', 'dp')), may hold values from 0 to 128, as said below
- dest: int32 [32, 4], P(('grp', 'dp')), may hold values from -1 to 3, as said below
- gain: float32 [3584], replicated, may hold values from 0.5 to 1.5
- weight: bfloat16 [3584, 10240], P('dp', 'grp'), may hold values from -0.09375 to 0.09375
Outputs:
- projected: bfloat16 [2048, 10240], P('dp', 'grp')
The draws below stay inside these ranges and needn't reach their ends.
Inputs may be any that keep to these rules, and one draw needn't show every extreme that they name: The tokens of one row have a common scale, and so have those of one feature. A device's live rows are the sum of its lengths; rows after them are padding. Within the devices sharing a dp index, live rows fill ceil(live rows / 32) blocks on each device and 8 blocks in all. dest is -1 exactly for a device's blocks past its live rows and an owner along grp otherwise. Within the devices sharing a dp index, every owner receives exactly 2 blocks and no device sends more than 1 block to one owner.
All inputs are finite; a program needn't handle non-finite values.
Results may differ from the reference program's by a relative error of at most 0.0049.
Values may be sent and summed in bfloat16 or wider, within the bound.
A program may use at most 64 MiB of HBM per device.

```python
import math
import jax
import jax.numpy as jnp
from jax import lax

D = 3584
FF = 10240
BLK = 32
DOCS = 4
OWN_BLK = 2
IN_BLK = 4
ROWS_GRP = 256
TOKENS = 4096
N_GRP = 4
N_DP = 8


def shared_layout(key):
    base = jax.random.fold_in(key, 7001)
    slots_in = 2 * OWN_BLK

    def one_group(group_key):
        keys = jax.random.split(group_key, 5)
        order = jax.random.permutation(keys[0], N_GRP)
        steps = jax.random.randint(keys[1], (N_GRP // 2,), 0, OWN_BLK + 1)
        steps = steps.at[0].set(OWN_BLK)
        delta = jnp.zeros((N_GRP,), jnp.int32)
        delta = delta.at[order[0::2]].set(steps).at[order[1::2]].set(-steps)
        counts = OWN_BLK + delta
        extra = jax.random.randint(keys[2], (N_GRP,), 1, BLK + 1)
        extra = extra.at[order[0]].set(BLK)
        live_rows = jnp.where(counts > 0, (counts - 1) * BLK + extra, 0)
        cuts = jax.random.randint(keys[3], (N_GRP, DOCS - 1), 0, live_rows[:, None] + 1)
        cuts = jnp.sort(cuts, axis=1)
        cuts = cuts.at[order[0]].set(0)
        bounds = jnp.concatenate([jnp.zeros((N_GRP, 1), jnp.int32), cuts, live_rows[:, None]], axis=1)
        lens = bounds[:, 1:] - bounds[:, :-1]
        owners = jax.random.permutation(keys[4], N_GRP)
        starts = jnp.cumsum(counts) - counts
        slot_index = jnp.arange(slots_in, dtype=jnp.int32)
        flat_pos = starts[:, None] + slot_index[None, :]
        dest = jnp.where(slot_index[None, :] < counts[:, None], owners[flat_pos % N_GRP], -1)
        return (lens.astype(jnp.int32), dest.astype(jnp.int32))
    group_keys = jax.random.split(base, N_DP)
    lens, dest = jax.vmap(one_group)(group_keys)
    lens = jnp.transpose(lens, (1, 0, 2)).reshape(N_GRP * N_DP, DOCS)
    dest = jnp.transpose(dest, (1, 0, 2)).reshape(N_GRP * N_DP, slots_in)
    return (lens, dest)


def draw_lengths(key, part):
    return shared_layout(key)[0]


def draw_dest(key, part):
    return shared_layout(key)[1]


def draw_tokens(key, part):
    keys = jax.random.split(jax.random.fold_in(key, 31), 3)
    values = jnp.clip(jax.random.normal(keys[0], (TOKENS, D), jnp.float32), -4.0, 4.0)
    row_scale = jnp.exp(jax.random.uniform(keys[1], (TOKENS, 1), jnp.float32, 0.0, math.log(10.0)))
    col_scale = jnp.exp(jax.random.uniform(keys[2], (1, D), jnp.float32, math.log(0.3), math.log(3.0)))
    return (values * row_scale * col_scale).astype(jnp.bfloat16)


def block_scale(own_key, extent, shards, least, high):
    loudness = 1.0
    for dim, parts in shards:
        heights = jax.random.uniform(jax.random.fold_in(jax.random.fold_in(own_key, 6), dim), (parts,), jnp.float32, least / len(shards), high / len(shards))
        loudness = loudness * jnp.repeat(jnp.exp(heights), extent[dim] // parts).reshape((-1,) + (1,) * (len(extent) - 1 - dim))
    return loudness


def noise(own_key, extent, deviation, most, cuts=(), held_as=jnp.bfloat16):
    loudness = block_scale(own_key, extent, cuts, -0.22, 0.18) if cuts else 1.0
    values = jax.random.normal(own_key, extent, jnp.float32) * deviation * loudness
    return jnp.minimum(jnp.maximum(values, -most), most).astype(held_as)


def setup_inputs(seed: int = 0) -> dict:
    key_list = jax.random.split(jax.random.key(seed), 6)
    return {
        "tokens": draw_tokens(jax.random.fold_in(key_list[5], 71), 0),
        "lengths": draw_lengths(jax.random.fold_in(key_list[5], 71), 0),
        "dest": draw_dest(jax.random.fold_in(key_list[5], 71), 0),
        "gain": jnp.clip(1.0 + 0.1 * jax.random.normal(key_list[3], (D,), jnp.float32), 0.5, 1.5),
        "weight": noise(key_list[4], (D, FF), D ** -0.5, 0.09375, ((0, 8), (1, 4))),
    }


EPS = 1e-06

def normalize_source(rows, lens, gain):
    count = rows.shape[0]
    doc_ends = jnp.cumsum(lens)
    position = jnp.arange(count, dtype=jnp.int32)
    doc_index = lax.optimization_barrier(jnp.sum((position[:, None] >= doc_ends[None, :]).astype(jnp.int32), axis=1))
    is_live = position < doc_ends[-1]
    onehot = (doc_index[:, None] == jnp.arange(DOCS, dtype=jnp.int32)[None, :]) & is_live[:, None]
    widened = rows.astype(jnp.float32)
    square = lax.optimization_barrier(jnp.sum(widened * widened, axis=1))
    totals = lax.optimization_barrier(jnp.sum(jnp.where(onehot, square[:, None], jnp.float32(0.0)), axis=0))
    mean_square = totals / (jnp.maximum(lens, 1).astype(jnp.float32) * D)
    inverse = lax.rsqrt(mean_square + EPS)
    scale = lax.optimization_barrier(jnp.sum(jnp.where(onehot, inverse[None, :], jnp.float32(0.0)), axis=1))
    return (widened * scale[:, None] * gain[None, :]).astype(jnp.bfloat16)

def group_rows(tokens_grp, lens_grp, dest_grp, gain):
    normed = jax.vmap(normalize_source, in_axes=(0, 0, None))(tokens_grp, lens_grp, gain)
    blocks = normed.reshape(N_GRP * IN_BLK, BLK, D)
    flat_dest = dest_grp.reshape(-1)
    flat_index = jnp.arange(N_GRP * IN_BLK, dtype=jnp.int32)
    earlier = (flat_dest[:, None] == flat_dest[None, :]) & (flat_index[None, :] < flat_index[:, None])
    owner_rank = lax.optimization_barrier(jnp.sum(earlier.astype(jnp.int32), axis=1))
    matches = (flat_dest[:, None, None] == jnp.arange(N_GRP, dtype=jnp.int32)[None, :, None]) & (owner_rank[:, None, None] == jnp.arange(OWN_BLK, dtype=jnp.int32)[None, None, :])
    picked = lax.optimization_barrier(jnp.sum(jnp.where(matches, flat_index[:, None, None], 0), axis=0)).astype(jnp.int32)
    chosen = blocks[picked.reshape(-1)]
    return chosen.reshape(ROWS_GRP, D)

def reference(tokens, lengths, dest, gain, weight):
    token_groups = jnp.transpose(tokens.reshape(N_GRP, N_DP, IN_BLK * BLK, D), (1, 0, 2, 3))
    length_groups = jnp.transpose(lengths.reshape(N_GRP, N_DP, DOCS), (1, 0, 2))
    dest_groups = jnp.transpose(dest.reshape(N_GRP, N_DP, IN_BLK), (1, 0, 2))

    def per_group(items):
        rows = group_rows(items[0], items[1], items[2], gain)
        return jnp.dot(rows, weight, preferred_element_type=jnp.float32).astype(jnp.bfloat16)
    result = lax.map(per_group, (token_groups, length_groups, dest_groups))
    return result.reshape(N_DP * ROWS_GRP, FF)
```

```python
import functools
import math

import jax
import jax.numpy as jnp
from jax import lax
from jax.experimental import pallas as pl
from jax.experimental.pallas import tpu as pltpu
from jax.sharding import PartitionSpec as P

BLK = 32
OWN_BLK = 2
EPS = 1e-06
MESH = pl.DeviceIdType.MESH


def kernel(cfg, lens_ref, dest_ref, tok_ref, gain_ref, w_ref, out_ref,
           wbuf, tbuf, gbuf, dbuf, abuf, acc, load_sem, ws, wr, zs, zr, ds_, dr):
    groups, side, pieces, features, split = cfg
    chips = side * side
    rows = w_ref.shape[0]
    cols = w_ref.shape[1]
    part = rows // pieces
    wide = 2 * rows
    mine = tbuf.shape[1]
    docs = lens_ref.shape[1]
    grp = lax.axis_index("grp")
    dp = lax.axis_index("dp")
    core = dp % 2
    lo = (dp // 2) % side
    hi = dp // (2 * side)

    def shard(c, dl, dh):
        return 2 * (((hi + dh) % side) * side + (lo + dl) % side) + c

    def first(c, j):
        return shard(c, j * (1 - c), j * c)

    def second(c, j):
        return shard(c, j * c, j * (1 - c))

    def corner(c, j, k):
        return shard(c, j * (1 - c) + k * c, j * c + k * (1 - c))

    sib = dp + 1 - 2 * core
    steps = range(1, side)
    edge = []
    for j in steps:
        edge.append((len(edge), "a", j, 0))
    for j in steps:
        edge.append((len(edge), "b", j, 0))
    diag = []
    for j in steps:
        for k in steps:
            diag.append((len(edge) + len(diag), "c", j, k))
    flows = len(edge) + len(diag)

    def origin(c, kind, j, k):
        if kind == "a":
            return first(c, side - j)
        if kind == "b":
            return second(c, side - j)
        return corner(c, side - j, side - k)

    def view(slot, q):
        return wbuf.at[pl.ds(pl.multiple_of(slot * rows + q * part, 16), part)]

    def wcopy(slot, q, idx, target):
        return pltpu.make_async_remote_copy(
            src_ref=view(slot, q), dst_ref=view(slot, q),
            send_sem=ws.at[idx, q], recv_sem=wr.at[idx, q],
            device_id={"dp": target}, device_id_type=MESH)

    def zview(src):
        return gbuf.at[src]

    def zcopies(way, s, src, target):
        return (
            pltpu.make_async_remote_copy(
                src_ref=zview(src), dst_ref=zview(src),
                send_sem=zs.at[way, s - 1], recv_sem=zr.at[way, s - 1],
                device_id={"grp": target}, device_id_type=MESH),
            pltpu.make_async_remote_copy(
                src_ref=dbuf.at[src], dst_ref=dbuf.at[src],
                send_sem=ds_.at[way, s - 1], recv_sem=dr.at[way, s - 1],
                device_id={"grp": target}, device_id_type=MESH),
        )

    load = pltpu.make_async_copy(
        w_ref, wbuf.at[pl.ds(pl.multiple_of(dp * rows, 16), rows)], load_sem.at[0])
    load.start()
    dload = pltpu.make_async_copy(dest_ref, dbuf.at[grp], load_sem.at[1])
    dload.start()

    barrier = pltpu.get_barrier_semaphore()
    for j in steps:
        pl.semaphore_signal(barrier, inc=1, device_id={"dp": first(core, j)}, device_id_type=MESH)
        pl.semaphore_signal(barrier, inc=1, device_id={"dp": second(core, j)}, device_id_type=MESH)
    pl.semaphore_signal(barrier, inc=1, device_id={"dp": sib}, device_id_type=MESH)

    @pl.when(grp > 0)
    def _():
        pl.semaphore_signal(barrier, inc=1, device_id={"grp": grp - 1}, device_id_type=MESH)

    @pl.when(grp < groups - 1)
    def _():
        pl.semaphore_signal(barrier, inc=1, device_id={"grp": grp + 1}, device_id_type=MESH)

    load.wait()
    ends = (grp + groups - 1) // groups + (2 * groups - 2 - grp) // groups
    pl.semaphore_wait(barrier, 2 * (side - 1) + 1 + ends)

    sent = []

    def go(copy):
        copy.start()
        sent.append(copy)

    for q in range(pieces):
        for n, kind, j, k in edge:
            go(wcopy(dp, q, n, first(core, j) if kind == "a" else second(core, j)))
        go(wcopy(dp, q, flows, sib))

    position = lax.broadcasted_iota(jnp.int32, (mine, 1), 0)
    square = jnp.zeros((mine, 1), jnp.float32)
    for h in range(chips):
        x = (tok_ref[h] if split else tok_ref[:, h * wide:(h + 1) * wide]).astype(jnp.float32)
        square = square + jnp.sum(x * x, axis=1, keepdims=True)
    scale = jnp.zeros((mine, 1), jnp.float32)
    end = jnp.int32(0)
    for c in range(docs):
        length = lens_ref[0, c]
        mask = (position >= end) & (position < end + length)
        total = jnp.sum(jnp.where(mask, square, 0.0), axis=0, keepdims=True)
        count = jnp.full((1, 1), jnp.maximum(length, 1), jnp.int32).astype(jnp.float32) * features
        scale = scale + jnp.where(mask, lax.rsqrt(total / count + EPS), 0.0)
        end = end + length
    for h in range(chips):
        x = (tok_ref[h] if split else tok_ref[:, h * wide:(h + 1) * wide]).astype(jnp.float32)
        g = gain_ref[h] if split else gain_ref[:, h * wide:(h + 1) * wide]
        tbuf[h] = (x * scale * g[0:1]).astype(jnp.bfloat16)
    tload = pltpu.make_async_copy(tbuf, zview(grp), load_sem.at[0])
    tload.start()
    dload.wait()
    tload.wait()

    def zsend(s):
        right = (grp - (s - 1) >= 0) & (grp < groups - 1)
        left = (grp + (s - 1) <= groups - 1) & (grp > 0)

        @pl.when(right)
        def _():
            for copy in zcopies(0, s, (grp - (s - 1) + groups) % groups, grp + 1):
                copy.start()

        @pl.when(left)
        def _():
            for copy in zcopies(1, s, (grp + (s - 1)) % groups, grp - 1):
                copy.start()

    def zrecv(s):
        @pl.when(grp - s >= 0)
        def _():
            for copy in zcopies(0, s, (grp - s + groups) % groups, grp):
                copy.wait_recv()

        @pl.when(grp + s <= groups - 1)
        def _():
            for copy in zcopies(1, s, (grp + s) % groups, grp):
                copy.wait_recv()

        if s < groups - 1:
            zsend(s + 1)

    def zdone(s):
        @pl.when((grp - (s - 1) >= 0) & (grp < groups - 1))
        def _():
            for copy in zcopies(0, s, (grp - (s - 1) + groups) % groups, grp):
                copy.wait_send()

        @pl.when((grp + (s - 1) <= groups - 1) & (grp > 0))
        def _():
            for copy in zcopies(1, s, (grp + (s - 1)) % groups, grp):
                copy.wait_send()

    zsend(1)

    def wrecv(entry, q):
        n, kind, j, k = entry
        slot = origin(core, kind, j, k)
        wcopy(slot, q, n, sib).wait_recv()
        if kind == "a":
            for far in steps:
                idx = len(edge) + (j - 1) * (side - 1) + far - 1
                go(wcopy(slot, q, idx, second(core, far)))
        go(wcopy(slot, q, flows + 1 + n, sib))

    def srecv(entry, q):
        if entry is None:
            wcopy(sib, q, flows, sib).wait_recv()
        else:
            n, kind, j, k = entry
            wcopy(origin(1 - core, kind, j, k), q, flows + 1 + n, sib).wait_recv()

    events = []
    for q in range(pieces):
        events.append((2.0 * (q + 1) / pieces, 0, functools.partial(
            lambda q: [wrecv(e, q) for e in edge], q)))
    for s in range(1, groups):
        events.append((0.8 * s, 1, functools.partial(zrecv, s)))
    events.sort(key=lambda e: e[:2])
    for _, _, act in events:
        act()

    out_rows = out_ref.shape[0]
    lane = lax.broadcasted_iota(jnp.int32, (8, mine), 1)
    slots_in = mine // BLK
    dests = [dbuf[g] for g in range(groups)]
    turned = [[d] + [pltpu.roll(d, BLK * t, 1) for t in range(1, slots_in)] for d in dests]
    row = lax.broadcasted_iota(jnp.int32, (out_rows, mine), 0)
    col = lax.broadcasted_iota(jnp.int32, (out_rows, mine), 1)
    same = (row % BLK) == (col % BLK)
    picks = []
    for g in range(groups):
        rank = jnp.zeros((8, mine), jnp.int32)
        for t in range(1, slots_in):
            rank = rank + jnp.where((turned[g][t] == dests[g]) & (lane >= BLK * t), 1, 0)
        for e in range(g):
            for t in range(slots_in):
                rank = rank + jnp.where(turned[e][t] == dests[g], 1, 0)
        place = jnp.where(dests[g] >= 0, dests[g] * OWN_BLK + rank, -1)
        hit = same & (place[0:1] == row // BLK)
        picks.append(jnp.where(hit, 1.0, 0.0).astype(jnp.bfloat16))
    pick = jnp.concatenate(picks, axis=1)

    @pl.loop(0, chips)
    def _(h):
        blocks = jnp.concatenate([gbuf[g, h] for g in range(groups)], axis=0)
        abuf[h] = jnp.dot(pick, blocks, preferred_element_type=jnp.float32).astype(jnp.bfloat16)

    tile = math.gcd(cols, 512)

    def chip_dot(chip, where):
        return jnp.dot(
            abuf[chip], wbuf[pl.ds(pl.multiple_of(chip * wide, 16), wide), where],
            preferred_element_type=jnp.float32)

    for q in range(pieces):
        for e in [None] + edge:
            srecv(e, q)

    near = [(0, 0)] + [(j, 0) for j in steps] + [(0, j) for j in steps]

    @pl.loop(0, cols // tile)
    def _(i):
        where = pl.ds(pl.multiple_of(i * tile, tile), tile)
        total = None
        for dl, dh in near:
            term = chip_dot(shard(0, dl, dh) // 2, where)
            total = term if total is None else total + term
        acc[:, where] = total

    for q in range(pieces):
        for e in diag:
            wrecv(e, q)
    for q in range(pieces):
        for e in diag:
            srecv(e, q)

    @pl.loop(0, cols // tile)
    def _(i):
        where = pl.ds(pl.multiple_of(i * tile, tile), tile)
        total = acc[:, where]
        for dl in steps:
            for dh in steps:
                total = total + chip_dot(shard(0, dl, dh) // 2, where)
        out_ref[:, where] = total.astype(out_ref.dtype)

    for copy in sent:
        copy.wait_send()
    for s in range(1, groups):
        zdone(s)


def per_device(sizes, tokens, lengths, dest, gain, weight):
    groups, n_dp = sizes
    chips = n_dp // 2
    side = math.isqrt(chips)
    assert side * side * 2 == n_dp
    mine, features = tokens.shape
    rows, cols = weight.shape
    wide = 2 * rows
    split = wide % 128 != 0
    pieces = 4 if rows % 64 == 0 else 1
    flows = side * side - 1
    if split:
        tokens = tokens.reshape(mine, chips, wide).transpose(1, 0, 2)
        gain = jnp.broadcast_to(gain.reshape(chips, 1, wide), (chips, 8, wide))
    else:
        gain = jnp.broadcast_to(gain.reshape(1, features), (8, features))
    dest_rows = jnp.broadcast_to(jnp.repeat(dest[0], BLK)[None, :], (8, mine))
    out_rows = groups * OWN_BLK * BLK
    vmem = pl.BlockSpec(memory_space=pltpu.VMEM)
    dma = pltpu.SemaphoreType.DMA
    return pl.pallas_call(
        functools.partial(kernel, (groups, side, pieces, features, split)),
        out_shape=jax.ShapeDtypeStruct((out_rows, cols), jnp.bfloat16),
        in_specs=[
            pl.BlockSpec(memory_space=pltpu.SMEM), vmem, vmem, vmem,
            pl.BlockSpec(memory_space=pl.ANY),
        ],
        out_specs=vmem,
        scratch_shapes=[
            pltpu.VMEM((n_dp * rows, cols), jnp.bfloat16),
            pltpu.VMEM((chips, mine, wide), jnp.bfloat16),
            pltpu.VMEM((groups, chips, mine, wide), jnp.bfloat16),
            pltpu.VMEM((groups, 8, mine), jnp.int32),
            pltpu.VMEM((chips, out_rows, wide), jnp.bfloat16),
            pltpu.VMEM((out_rows, cols), jnp.float32),
            dma((2,)),
            dma((2 * flows + 1, pieces)),
            dma((2 * flows + 1, pieces)),
            dma((2, groups - 1)),
            dma((2, groups - 1)),
            dma((2, groups - 1)),
            dma((2, groups - 1)),
        ],
        compiler_params=pltpu.CompilerParams(
            collective_id=0, has_side_effects=True, vmem_limit_bytes=62 * 2**20),
    )(lengths, dest_rows, tokens, gain, weight)


def solution(mesh):
    placed = (
        P(("grp", "dp"), None),
        P(("grp", "dp"), None),
        P(("grp", "dp"), None),
        P(),
        P("dp", "grp"),
    )
    sizes = (mesh.shape["grp"], mesh.shape["dp"])
    return jax.shard_map(
        functools.partial(per_device, sizes), mesh=mesh, in_specs=placed,
        out_specs=P("dp", "grp"), check_vma=False
    )
```
